32 devices in a mesh: gx: 4 (over y, x), gy: 4 (over z), gz: 2 (over core).
Axes of the slice: x: 2, y: 2, z: 4, core: 2. Of those that a mesh axis runs over, the one named last changes fastest.
Arguments:
- blocks: int32 [32768, 4], P(('gx', 'gy', 'gz')), may hold values from 0 to 15, as said below
- coefficients: bfloat16 [32768, 4, 128], P(('gx', 'gy', 'gz')), may hold values from -80 to 80
- residuals: float32 [32768], P(('gx', 'gy', 'gz')), may hold values from -3000 to 3000
Outputs:
- factor: float32 [4, 4, 128, 4, 4, 128], P('gx', None, None, 'gy')
- solution: float32 [16, 128], replicated
The draws below stay inside these ranges and needn't reach their ends.
Inputs may be any that keep to these rules, and one draw needn't show every extreme that they name: Each row names 4 different blocks.
All inputs are finite; a program needn't handle non-finite values.
Results may differ from the reference program's by a relative error of at most 0.0003.
Values sent between devices are 32-bit elements; how exact they have to be, the bound alone decides.
A program may use at most 128 MiB of HBM per device.

```python
import math
import jax
import jax.numpy as jnp
from jax import lax

G = 2048
BS = 128
SLOTS = 4
OBS = 32768
N_GX = 4
N_GY = 4


def pick_blocks(key):
    nblock = G // BS
    base = jax.random.fold_in(key, 11)
    scores = jax.random.randint(base, (OBS, nblock), 0, 1 << 20) * nblock + jnp.arange(nblock, dtype=jnp.int32)[None, :]
    chosen = lax.top_k(scores, SLOTS)[1]
    return chosen.astype(jnp.int32)


def make_coefficients(key):
    base = jax.random.fold_in(key, 23)
    noise = jnp.clip(jax.random.normal(jax.random.fold_in(base, 1), (OBS, SLOTS, BS), jnp.float32), -6.0, 6.0)
    mixing = jax.random.normal(jax.random.fold_in(base, 3), (BS, BS), jnp.float32) / math.sqrt(BS)
    neighbour = jnp.roll(noise, -1, axis=1)
    coupled = noise + 0.35 * jnp.einsum('osx,xy->osy', neighbour, mixing)
    return jnp.clip(coupled, -80.0, 80.0)


def draw_blocks(key, part):
    return pick_blocks(key)


def draw_coefficients(key, part):
    return make_coefficients(key).astype(jnp.bfloat16)


def draw_residuals(key, part):
    coef = make_coefficients(key)
    chosen = pick_blocks(key)
    truth = jax.random.normal(jax.random.fold_in(key, 37), (G // BS, BS), jnp.float32)
    picked = truth[chosen]
    noise = jax.random.normal(jax.random.fold_in(key, 41), (OBS,), jnp.float32)
    values = jnp.sum(coef * picked, axis=(1, 2)) + noise
    return jnp.clip(values, -3000.0, 3000.0)


def setup_inputs(seed: int = 0) -> dict:
    key_list = jax.random.split(jax.random.key(seed), 4)
    blocks = draw_blocks(jax.random.fold_in(key_list[3], 71), 0)
    coefficients = draw_coefficients(jax.random.fold_in(key_list[3], 71), 0)
    residuals = draw_residuals(jax.random.fold_in(key_list[3], 71), 0)
    return {"blocks": blocks, "coefficients": coefficients, "residuals": residuals}


def reference(blocks, coefficients, residuals):
    total = blocks.shape[0]
    nblock = G // BS
    per_dev = nblock // N_GX
    group = math.gcd(total, 4096)
    count = total // group
    labels = jnp.arange(nblock, dtype=jnp.int32)

    def accumulate(carry, index):
        start = (index * group).astype(jnp.int32)
        picked = lax.dynamic_slice_in_dim(blocks, start, group, 0)
        coef = lax.dynamic_slice_in_dim(coefficients, start, group, 0).astype(jnp.float32)
        resid = lax.dynamic_slice_in_dim(residuals, start, group, 0)
        placed = (picked[:, :, None] == labels[None, None, :]).astype(jnp.float32)
        design = jnp.einsum('osa,osx->oax', placed, coef, precision=lax.Precision.HIGHEST).reshape(group, G)
        normal = carry[0] + jnp.dot(design.T.astype(jnp.float32), design.astype(jnp.float32), precision=lax.Precision.HIGHEST, preferred_element_type=jnp.float32)
        rhs = carry[1] + jnp.dot(resid.astype(jnp.float32), design.astype(jnp.float32), precision=lax.Precision.HIGHEST, preferred_element_type=jnp.float32)
        return ((normal, rhs), None)
    start_state = (jnp.zeros((G, G), jnp.float32), jnp.zeros((G,), jnp.float32))
    (normal, rhs), _ = lax.scan(accumulate, start_state, jnp.arange(count, dtype=jnp.int32))
    normal = normal / total
    rhs = rhs / total
    lower = jnp.linalg.cholesky(normal)
    middle = jax.scipy.linalg.solve_triangular(lower, rhs, lower=True)
    answer = jax.scipy.linalg.solve_triangular(lower.T, middle, lower=False)
    factor = lower.reshape(per_dev, N_GX, BS, per_dev, N_GY, BS).transpose(1, 0, 2, 4, 3, 5)
    return (factor, answer.reshape(nblock, BS))
```

```python
import functools

import jax
import jax.numpy as jnp
from jax import lax
from jax.experimental import pallas as pl
from jax.experimental.pallas import tpu as pltpu
from jax.sharding import PartitionSpec as P

G = 2048
BS = 128
SB = 2 * BS
SUB = 8
VMEM_LIMIT = 60 * 1024 * 1024


def mm(a, b, ca, cb, precision=lax.Precision.HIGHEST):
    return lax.dot_general(
        a, b, (((ca,), (cb,)), ((), ())), precision=precision, preferred_element_type=jnp.float32
    )


def panel_start(nblock, k):
    return BS * (nblock * k - (k * (k - 1)) // 2)


def gram_kernel(nblock, scale, blocks_ref, coef_ref, res_ref, out_ref, design):
    slots = coef_ref.shape[0]
    rows = coef_ref.shape[1]
    chunk = 128
    nsuper = nblock // 2

    @pl.loop(0, rows // chunk)
    def _(t):
        at = pl.ds(pl.multiple_of(t * chunk, chunk), chunk)
        idx = blocks_ref[at, :]
        labels = [jnp.broadcast_to(idx[:, s : s + 1], (chunk, BS)) for s in range(slots)]
        values = [coef_ref[s, at, :].astype(jnp.float32) for s in range(slots)]
        for b in range(nblock):
            total = jnp.where(labels[0] == b, values[0], 0.0)
            for s in range(1, slots):
                total = jnp.where(labels[s] == b, values[s], total)
            design[at, b * BS : (b + 1) * BS] = total.astype(jnp.bfloat16)

    res = res_ref[...]
    high = res.astype(jnp.bfloat16)
    rest = res - high.astype(jnp.float32)
    mid = rest.astype(jnp.bfloat16)
    low = (rest - mid.astype(jnp.float32)).astype(jnp.bfloat16)
    row = lax.broadcasted_iota(jnp.int32, (16, rows), 0)
    parts = jnp.where(
        row == 0,
        high.astype(jnp.float32),
        jnp.where(
            row == 1,
            mid.astype(jnp.float32),
            jnp.where(row == 2, low.astype(jnp.float32), 0.0),
        ),
    ).astype(jnp.bfloat16)
    base = panel_start(nblock, nblock)
    out_ref[base:, :] = jnp.zeros((out_ref.shape[0] - base, BS), jnp.float32)
    for b in range(nblock):
        part = mm(parts, design[:, b * BS : (b + 1) * BS], 1, 0, None)
        out_ref[base + b : base + b + 1, :] = jnp.sum(part, axis=0, keepdims=True) * scale

    @pl.loop(0, nsuper)
    def _(jj):
        right = design[:, pl.ds(pl.multiple_of(jj * SB, SB), SB)]
        first = pl.multiple_of(panel_start(nblock, 2 * jj), BS)
        second = pl.multiple_of(panel_start(nblock, 2 * jj + 1), BS)
        block = mm(right, right, 0, 0, None) * scale
        out_ref[pl.ds(first, SB), :] = block[:, :BS]
        out_ref[pl.ds(second, BS), :] = block[BS:, BS:]

        @pl.loop(jj + 1, nsuper)
        def _(ii):
            left = design[:, pl.ds(pl.multiple_of(ii * SB, SB), SB)]
            block = mm(left, right, 0, 0, None) * scale
            down = (ii - jj) * SB
            out_ref[pl.ds(pl.multiple_of(first + down, BS), SB), :] = block[:, :BS]
            out_ref[pl.ds(pl.multiple_of(second + down - BS, BS), SB), :] = block[:, BS:]


def factor_diag(a, e):
    sub = lax.broadcasted_iota(jnp.int32, (SUB, BS), 0)
    shape = (SUB, BS)
    count = BS // SUB

    def lane(x, j):
        return jnp.broadcast_to(x[:, j : j + 1], shape)

    def sublane(x, j):
        return jnp.broadcast_to(x[j : j + 1, :], shape)

    for p in range(count):
        base = p * SUB
        block = a[base : base + SUB, :]
        eblock = e[base : base + SUB, :]
        cols = [lane(block, base + j) for j in range(SUB)]
        scales, rows, erows, upper = [], [], [], {}
        for j in range(SUB):
            inv = lax.rsqrt(sublane(cols[j], j))
            scales.append(inv)
            mult = jnp.where(sub > j, cols[j] * inv, 0.0)
            for k in range(j + 1, SUB):
                upper[j, k] = sublane(cols[k], j) * inv
                cols[k] = cols[k] - mult * upper[j, k]
            row = sublane(block, j) * inv
            erow = sublane(eblock, j) * inv
            block = jnp.where(sub == j, row, block - mult * row)
            eblock = jnp.where(sub == j, erow, eblock - mult * erow)
            rows.append(row)
            erows.append(erow)
        a[base : base + SUB, :] = block
        e[base : base + SUB, :] = eblock
        for i in range(p + 1, count):
            at = slice(i * SUB, (i + 1) * SUB)
            below = a[at, :]
            ebelow = e[at, :]
            cols = [lane(below, base + j) for j in range(SUB)]
            for j in range(SUB):
                mult = cols[j] * scales[j]
                for k in range(j + 1, SUB):
                    cols[k] = cols[k] - mult * upper[j, k]
                below = below - mult * rows[j]
                ebelow = ebelow - mult * erows[j]
            a[at, :] = below
            e[at, :] = ebelow


def factor_kernel(nblock, place_ref, packed_ref, factor_ref, z_ref, w, inverse, a, e, y, sems):
    nsuper = nblock // 2
    size = nblock * BS
    base = panel_start(nblock, nblock)
    copies = []
    for k in range(nblock):
        begin = panel_start(nblock, k)
        copies.append(
            pltpu.make_async_copy(
                packed_ref.at[begin : begin + size - k * BS, :],
                w.at[k, k * BS : size, :],
                sems.at[k],
            )
        )
    copies.append(
        pltpu.make_async_copy(packed_ref.at[base : base + nblock, :], z_ref, sems.at[nblock])
    )
    for copy in copies:
        copy.start()
    for copy in copies:
        copy.wait()
    y[...] = jnp.zeros_like(y)
    for b in range(nblock):
        y[b // 2, 0:1, (b % 2) * BS : (b % 2 + 1) * BS] = z_ref[b : b + 1, :]
    row = lax.broadcasted_iota(jnp.int32, (BS, BS), 0)
    col = lax.broadcasted_iota(jnp.int32, (BS, BS), 1)
    eye = jnp.where(row == col, 1.0, 0.0).astype(jnp.float32)

    def wide(k, start, height):
        at = pl.ds(pl.multiple_of(start, BS), height)
        return jnp.concatenate([w[2 * k, at, :], w[2 * k + 1, at, :]], axis=1)

    @pl.loop(0, nsuper)
    def _(kk):
        top = pl.ds(pl.multiple_of(kk * SB, BS), BS)
        low = pl.ds(pl.multiple_of(kk * SB + BS, BS), BS)
        k = 2 * kk
        l21 = None
        e1 = None
        for half in range(2):
            if half == 0:
                a[...] = w[k, top, :]
            else:
                l21 = mm(w[k, low, :], e1, 1, 1)
                w[k, low, :] = l21
                a[...] = w[k + 1, low, :] - mm(l21, l21, 1, 1)
            e[...] = eye
            factor_diag(a, e)
            chol = jnp.where(row <= col, a[...], 0.0).T
            if half == 0:
                w[k, top, :] = chol
                e1 = jnp.where(row >= col, e[...], 0.0)
                inverse[kk, 0:BS, 0:BS] = e1
                inverse[kk, 0:BS, BS:SB] = jnp.zeros((BS, BS), jnp.float32)
            else:
                w[k + 1, low, :] = chol
                e2 = jnp.where(row >= col, e[...], 0.0)
                inverse[kk, BS:SB, BS:SB] = e2
                inverse[kk, BS:SB, 0:BS] = -mm(e2, mm(l21, e1, 1, 0), 1, 0)
        y[kk] = mm(y[kk], inverse[kk], 1, 1)

        @pl.loop(kk + 1, nsuper)
        def _(ii):
            at = pl.ds(pl.multiple_of(ii * SB, BS), SB)
            panel = mm(wide(kk, ii * SB, SB), inverse[kk], 1, 1)
            w[k, at, :] = panel[:, :BS]
            w[k + 1, at, :] = panel[:, BS:]

        @pl.loop(kk + 1, nsuper)
        def _(jj):
            right = wide(kk, jj * SB, SB)
            y[jj] = y[jj] - mm(y[kk], right, 1, 1)

            @pl.loop(jj, nsuper)
            def _(ii):
                at = pl.ds(pl.multiple_of(ii * SB, BS), SB)
                update = mm(wide(kk, ii * SB, SB), right, 1, 1)
                w[2 * jj, at, :] = w[2 * jj, at, :] - update[:, :BS]
                w[2 * jj + 1, at, :] = w[2 * jj + 1, at, :] - update[:, BS:]

    @pl.loop(0, nsuper)
    def _(step):
        kk = nsuper - 1 - step

        def body(ii, total):
            return total - mm(y[ii], wide(kk, ii * SB, SB), 1, 0)

        total = lax.fori_loop(kk + 1, nsuper, body, y[kk])
        y[kk] = mm(total, inverse[kk], 1, 0)

    for b in range(nblock):
        z_ref[b : b + 1, :] = y[b // 2, 0:1, (b % 2) * BS : (b % 2 + 1) * BS]

    per_row, per_col = factor_ref.shape[0], factor_ref.shape[2] // BS
    rows_of, cols_of = nblock // per_row, nblock // per_col
    for r in range(per_row):
        for c in range(per_col):
            rb = r * rows_of + place_ref[0]
            cb = c * cols_of + place_ref[1]
            block = w[cb, pl.ds(pl.multiple_of(rb * BS, BS), BS), :]
            keep = row + rb * BS >= col + cb * BS
            factor_ref[r, :, c * BS : (c + 1) * BS] = jnp.where(keep, block, 0.0)


def on_device(blocks, coefficients, residuals):
    row_count = lax.axis_size("gx")
    col_count = lax.axis_size("gy")
    axes = ("gx", "gy", "gz")
    devices = row_count * col_count * lax.axis_size("gz")
    rows, slots, width = coefficients.shape
    scale = 1.0 / (rows * devices)
    nblock = G // width
    nsuper = nblock // 2
    used = panel_start(nblock, nblock) + nblock
    total = -(-used // (SUB * devices)) * SUB * devices
    vmem = pl.BlockSpec(memory_space=pltpu.VMEM)
    term = pl.pallas_call(
        functools.partial(gram_kernel, nblock, scale),
        out_shape=jax.ShapeDtypeStruct((total, width), jnp.float32),
        in_specs=[vmem] * 3,
        out_specs=vmem,
        scratch_shapes=[pltpu.VMEM((rows, G), jnp.bfloat16)],
        compiler_params=pltpu.CompilerParams(vmem_limit_bytes=VMEM_LIMIT),
    )(blocks, coefficients.transpose(1, 0, 2), residuals.reshape(1, rows))
    part = lax.psum_scatter(term, axes, scatter_dimension=0, tiled=True)
    packed = lax.all_gather(part, axes, axis=0, tiled=True)
    place = jnp.stack([lax.axis_index("gx"), lax.axis_index("gy")]).astype(jnp.int32)
    per_row, per_col = nblock // row_count, nblock // col_count
    factor, answer = pl.pallas_call(
        functools.partial(factor_kernel, nblock),
        out_shape=(
            jax.ShapeDtypeStruct((per_row, width, per_col * width), jnp.float32),
            jax.ShapeDtypeStruct((nblock, width), jnp.float32),
        ),
        in_specs=[pl.BlockSpec(memory_space=pltpu.SMEM), pl.BlockSpec(memory_space=pl.ANY)],
        out_specs=(vmem, vmem),
        scratch_shapes=[
            pltpu.VMEM((nblock, G, width), jnp.float32),
            pltpu.VMEM((nsuper, SB, SB), jnp.float32),
            pltpu.VMEM((width, width), jnp.float32),
            pltpu.VMEM((width, width), jnp.float32),
            pltpu.VMEM((nsuper, SUB, SB), jnp.float32),
            pltpu.SemaphoreType.DMA((nblock + 1,)),
        ],
        compiler_params=pltpu.CompilerParams(vmem_limit_bytes=VMEM_LIMIT),
    )(place, packed)
    return (factor.reshape(1, per_row, width, 1, per_col, width), answer)


def solution(mesh):
    in_specs = (
        P(("gx", "gy", "gz"), None),
        P(("gx", "gy", "gz"), None, None),
        P(("gx", "gy", "gz")),
    )
    out_specs = (P("gx", None, None, "gy", None, None), P())
    return jax.shard_map(
        on_device, mesh=mesh, in_specs=in_specs, out_specs=out_specs, check_vma=False
    )
```

```python
import functools

import jax
import jax.numpy as jnp
from jax import lax
from jax.experimental import pallas as pl
from jax.experimental.pallas import tpu as pltpu
from jax.sharding import PartitionSpec as P

G = 2048
BS = 128
SB = 2 * BS
SUB = 8
VMEM_LIMIT = 60 * 1024 * 1024


def mm(a, b, ca, cb, precision=lax.Precision.HIGHEST):
    return lax.dot_general(
        a, b, (((ca,), (cb,)), ((), ())), precision=precision, preferred_element_type=jnp.float32
    )


def split(x):
    high = x.astype(jnp.bfloat16)
    return high, (x - high.astype(jnp.float32)).astype(jnp.bfloat16)


def mm3(a, b, ca, cb):
    (ah, al), (bh, bl) = split(a), b if isinstance(b, tuple) else split(b)
    return mm(ah, bh, ca, cb, None) + (mm(ah, bl, ca, cb, None) + mm(al, bh, ca, cb, None))


def panel_start(nblock, k):
    return BS * (nblock * k - (k * (k - 1)) // 2)


def gram_kernel(nblock, scale, blocks_ref, coef_ref, res_ref, out_ref, design):
    slots = coef_ref.shape[0]
    rows = coef_ref.shape[1]
    chunk = 128
    nsuper = nblock // 2

    @pl.loop(0, rows // chunk)
    def _(t):
        at = pl.ds(pl.multiple_of(t * chunk, chunk), chunk)
        idx = blocks_ref[at, :]
        labels = [jnp.broadcast_to(idx[:, s : s + 1], (chunk, BS)) for s in range(slots)]
        values = [coef_ref[s, at, :].astype(jnp.float32) for s in range(slots)]
        for b in range(nblock):
            total = jnp.where(labels[0] == b, values[0], 0.0)
            for s in range(1, slots):
                total = jnp.where(labels[s] == b, values[s], total)
            design[at, b * BS : (b + 1) * BS] = total.astype(jnp.bfloat16)

    res = res_ref[...]
    high = res.astype(jnp.bfloat16)
    rest = res - high.astype(jnp.float32)
    mid = rest.astype(jnp.bfloat16)
    low = (rest - mid.astype(jnp.float32)).astype(jnp.bfloat16)
    row = lax.broadcasted_iota(jnp.int32, (16, rows), 0)
    parts = jnp.where(
        row == 0,
        high.astype(jnp.float32),
        jnp.where(
            row == 1,
            mid.astype(jnp.float32),
            jnp.where(row == 2, low.astype(jnp.float32), 0.0),
        ),
    ).astype(jnp.bfloat16)
    base = panel_start(nblock, nblock)
    out_ref[base:, :] = jnp.zeros((out_ref.shape[0] - base, BS), jnp.float32)
    for b in range(nblock):
        part = mm(parts, design[:, b * BS : (b + 1) * BS], 1, 0, None)
        out_ref[base + b : base + b + 1, :] = jnp.sum(part, axis=0, keepdims=True) * scale

    @pl.loop(0, nsuper)
    def _(jj):
        right = design[:, pl.ds(pl.multiple_of(jj * SB, SB), SB)]
        first = pl.multiple_of(panel_start(nblock, 2 * jj), BS)
        second = pl.multiple_of(panel_start(nblock, 2 * jj + 1), BS)
        block = mm(right, right, 0, 0, None) * scale
        out_ref[pl.ds(first, SB), :] = block[:, :BS]
        out_ref[pl.ds(second, BS), :] = block[BS:, BS:]

        @pl.loop(jj + 1, nsuper)
        def _(ii):
            left = design[:, pl.ds(pl.multiple_of(ii * SB, SB), SB)]
            block = mm(left, right, 0, 0, None) * scale
            down = (ii - jj) * SB
            out_ref[pl.ds(pl.multiple_of(first + down, BS), SB), :] = block[:, :BS]
            out_ref[pl.ds(pl.multiple_of(second + down - BS, BS), SB), :] = block[:, BS:]


def factor_diag(a, e):
    sub = lax.broadcasted_iota(jnp.int32, (SUB, BS), 0)
    shape = (SUB, BS)
    count = BS // SUB

    def lane(x, j):
        return jnp.broadcast_to(x[:, j : j + 1], shape)

    def sublane(x, j):
        return jnp.broadcast_to(x[j : j + 1, :], shape)

    for p in range(count):
        base = p * SUB
        block = a[base : base + SUB, :]
        eblock = e[base : base + SUB, :]
        cols = [lane(block, base + j) for j in range(SUB)]
        scales, rows, erows, upper = [], [], [], {}
        for j in range(SUB):
            inv = lax.rsqrt(sublane(cols[j], j))
            scales.append(inv)
            mult = jnp.where(sub > j, cols[j] * inv, 0.0)
            for k in range(j + 1, SUB):
                upper[j, k] = sublane(cols[k], j) * inv
                cols[k] = cols[k] - mult * upper[j, k]
            row = sublane(block, j) * inv
            erow = sublane(eblock, j) * inv
            block = jnp.where(sub == j, row, block - mult * row)
            eblock = jnp.where(sub == j, erow, eblock - mult * erow)
            rows.append(row)
            erows.append(erow)
        a[base : base + SUB, :] = block
        e[base : base + SUB, :] = eblock
        for i in range(p + 1, count):
            at = slice(i * SUB, (i + 1) * SUB)
            below = a[at, :]
            ebelow = e[at, :]
            cols = [lane(below, base + j) for j in range(SUB)]
            for j in range(SUB):
                mult = cols[j] * scales[j]
                for k in range(j + 1, SUB):
                    cols[k] = cols[k] - mult * upper[j, k]
                below = below - mult * rows[j]
                ebelow = ebelow - mult * erows[j]
            a[at, :] = below
            e[at, :] = ebelow


def factor_kernel(nblock, place_ref, packed_ref, factor_ref, z_ref, w, inverse, a, e, y, sems):
    nsuper = nblock // 2
    size = nblock * BS
    base = panel_start(nblock, nblock)
    copies = []
    for k in range(nblock):
        begin = panel_start(nblock, k)
        copies.append(
            pltpu.make_async_copy(
                packed_ref.at[begin : begin + size - k * BS, :],
                w.at[k, k * BS : size, :],
                sems.at[k],
            )
        )
    copies.append(
        pltpu.make_async_copy(packed_ref.at[base : base + nblock, :], z_ref, sems.at[nblock])
    )
    for copy in copies:
        copy.start()
    for copy in copies:
        copy.wait()
    y[...] = jnp.zeros_like(y)
    for b in range(nblock):
        y[b // 2, 0:1, (b % 2) * BS : (b % 2 + 1) * BS] = z_ref[b : b + 1, :]
    row = lax.broadcasted_iota(jnp.int32, (BS, BS), 0)
    col = lax.broadcasted_iota(jnp.int32, (BS, BS), 1)
    eye = jnp.where(row == col, 1.0, 0.0).astype(jnp.float32)

    def wide(k, start, height):
        at = pl.ds(pl.multiple_of(start, BS), height)
        return jnp.concatenate([w[2 * k, at, :], w[2 * k + 1, at, :]], axis=1)

    @pl.loop(0, nsuper)
    def _(kk):
        top = pl.ds(pl.multiple_of(kk * SB, BS), BS)
        low = pl.ds(pl.multiple_of(kk * SB + BS, BS), BS)
        k = 2 * kk
        l21 = None
        e1 = None
        for half in range(2):
            if half == 0:
                a[...] = w[k, top, :]
            else:
                l21 = mm(w[k, low, :], e1, 1, 1)
                w[k, low, :] = l21
                a[...] = w[k + 1, low, :] - mm(l21, l21, 1, 1)
            e[...] = eye
            factor_diag(a, e)
            chol = jnp.where(row <= col, a[...], 0.0).T
            if half == 0:
                w[k, top, :] = chol
                e1 = jnp.where(row >= col, e[...], 0.0)
                inverse[kk, 0:BS, 0:BS] = e1
                inverse[kk, 0:BS, BS:SB] = jnp.zeros((BS, BS), jnp.float32)
            else:
                w[k + 1, low, :] = chol
                e2 = jnp.where(row >= col, e[...], 0.0)
                inverse[kk, BS:SB, BS:SB] = e2
                inverse[kk, BS:SB, 0:BS] = -mm(e2, mm(l21, e1, 1, 0), 1, 0)
        y[kk] = mm(y[kk], inverse[kk], 1, 1)

        @pl.loop(kk + 1, nsuper)
        def _(ii):
            at = pl.ds(pl.multiple_of(ii * SB, BS), SB)
            panel = mm3(wide(kk, ii * SB, SB), inverse[kk], 1, 1)
            w[k, at, :] = panel[:, :BS]
            w[k + 1, at, :] = panel[:, BS:]

        @pl.loop(kk + 1, nsuper)
        def _(jj):
            right = split(wide(kk, jj * SB, SB))
            y[jj] = y[jj] - mm3(y[kk], right, 1, 1)

            @pl.loop(jj, nsuper)
            def _(ii):
                at = pl.ds(pl.multiple_of(ii * SB, BS), SB)
                update = mm3(wide(kk, ii * SB, SB), right, 1, 1)
                w[2 * jj, at, :] = w[2 * jj, at, :] - update[:, :BS]
                w[2 * jj + 1, at, :] = w[2 * jj + 1, at, :] - update[:, BS:]

    @pl.loop(0, nsuper)
    def _(step):
        kk = nsuper - 1 - step

        def body(ii, total):
            return total - mm3(y[ii], wide(kk, ii * SB, SB), 1, 0)

        total = lax.fori_loop(kk + 1, nsuper, body, y[kk])
        y[kk] = mm(total, inverse[kk], 1, 0)

    for b in range(nblock):
        z_ref[b : b + 1, :] = y[b // 2, 0:1, (b % 2) * BS : (b % 2 + 1) * BS]

    per_row, per_col = factor_ref.shape[0], factor_ref.shape[2] // BS
    rows_of, cols_of = nblock // per_row, nblock // per_col
    for r in range(per_row):
        for c in range(per_col):
            rb = r * rows_of + place_ref[0]
            cb = c * cols_of + place_ref[1]
            block = w[cb, pl.ds(pl.multiple_of(rb * BS, BS), BS), :]
            keep = row + rb * BS >= col + cb * BS
            factor_ref[r, :, c * BS : (c + 1) * BS] = jnp.where(keep, block, 0.0)


def exchange_kernel(nx, ny, n_gz, term_ref, out_ref, halves, stage, slots, s1, r1, s2, r2, s3, r3, s4, r4):
    n = nx * ny
    mp, mq = lax.axis_index("gx"), lax.axis_index("gy")
    me = mp * ny + mq
    g = lax.axis_index("gz")

    def remote(src, dst, send, recv, device):
        return pltpu.make_async_remote_copy(
            src_ref=src,
            dst_ref=dst,
            send_sem=send,
            recv_sem=recv,
            device_id=device,
            device_id_type=pl.DeviceIdType.MESH,
        )

    def half(c, d):
        peer = lax.rem(g + d, n_gz)
        return remote(
            term_ref.at[c, peer],
            halves.at[d - 1, c],
            s1.at[d - 1, c],
            r1.at[d - 1, c],
            {"gz": peer},
        )

    def to_row(p, q, slot):
        at, to = p * ny + q, slot * ny + q
        return remote(stage.at[at], slots.at[to], s2.at[at], r2.at[to], {"gx": p})

    def to_owner(q, slot):
        at, to = mp * ny + q, mp * ny + slot
        return remote(stage.at[at], slots.at[to], s2.at[at], r2.at[to], {"gy": q})

    def out_cols(q, owner):
        at = mp * ny + owner
        block = out_ref.at[at, g]
        return remote(block, block, s3.at[mp * ny + q], r3.at[at], {"gy": q})

    def out_rows(p, q, owner):
        at = owner * ny + q
        block = out_ref.at[at, g]
        return remote(block, block, s3.at[p * ny + q], r3.at[at], {"gx": p})

    def across(c, d, layer):
        block = out_ref.at[c, layer]
        return remote(
            block, block, s4.at[d - 1, c], r4.at[d - 1, c], {"gz": lax.rem(g + d, n_gz)}
        )

    def combine(c):
        total = term_ref[c, g]
        for d in range(1, n_gz):
            half(c, d).wait_recv()
            total = total + halves[d - 1, c]
        return total

    @pl.loop(0, n)
    def _(i):
        q = lax.rem(mq + 1 + i // nx, ny)
        p = lax.rem(mp + 1 + i % nx, nx)
        for d in range(1, n_gz):
            half(p * ny + q, d).start()

    @pl.loop(0, ny)
    def _(i):
        q = lax.rem(mq + 1 + i, ny)

        @pl.loop(0, nx - 1)
        def _(j):
            p = lax.rem(mp + 1 + j, nx)
            stage[p * ny + q] = combine(p * ny + q)
            to_row(p, q, mp).start()

    def row_sum(q):
        at = mp * ny + q
        stage[at] = combine(at)

        @pl.loop(0, nx - 1)
        def _(j):
            p = lax.rem(mp + nx - 1 - j, nx)
            to_row(p, q, p).wait_recv()
            stage[at] = stage[at] + slots[p * ny + q]

    @pl.loop(0, ny - 1)
    def _(i):
        q = lax.rem(mq + 1 + i, ny)
        row_sum(q)
        to_owner(q, mq).start()

    row_sum(mq)
    out_ref[me, g] = stage[me]

    @pl.loop(0, ny - 1)
    def _(i):
        q = lax.rem(mq + ny - 1 - i, ny)
        to_owner(q, q).wait_recv()
        out_ref[me, g] = out_ref[me, g] + slots[mp * ny + q]

    def spread(q):
        @pl.loop(0, nx - 1)
        def _(j):
            out_rows(lax.rem(mp + 1 + j, nx), q, mp).start()

        for d in range(1, n_gz):
            across(mp * ny + q, d, g).start()

    @pl.loop(0, ny - 1)
    def _(i):
        out_cols(lax.rem(mq + 1 + i, ny), mq).start()

    spread(mq)

    @pl.loop(0, ny - 1)
    def _(i):
        q = lax.rem(mq + ny - 1 - i, ny)
        out_cols(q, q).wait_recv()
        spread(q)

    @pl.loop(0, ny)
    def _(i):
        q = lax.rem(mq + ny - i, ny)

        @pl.loop(0, nx - 1)
        def _(j):
            p = lax.rem(mp + nx - 1 - j, nx)
            out_rows(p, q, p).wait_recv()
            for d in range(1, n_gz):
                across(p * ny + q, d, g).start()

    @pl.loop(0, n)
    def _(c):
        for d in range(1, n_gz):
            across(c, d, lax.rem(g + n_gz - d, n_gz)).wait_recv()
            across(c, d, g).wait_send()
            half(c, d).wait_send()

    @pl.loop(0, ny)
    def _(q):
        @pl.loop(0, nx - 1)
        def _(j):
            p = lax.rem(mp + 1 + j, nx)
            to_row(p, q, mp).wait_send()
            out_rows(p, q, mp).wait_send()

    @pl.loop(0, ny - 1)
    def _(i):
        q = lax.rem(mq + 1 + i, ny)
        to_owner(q, mq).wait_send()
        out_cols(q, mq).wait_send()


def exchange(term, row_count, col_count, n_gz):
    n = row_count * col_count
    total, width = term.shape
    part = total // (n * n_gz)
    shape = (n, n_gz, part, width)
    vmem = pl.BlockSpec(memory_space=pltpu.VMEM)
    pair = pltpu.SemaphoreType.DMA((n_gz - 1, n))
    single = pltpu.SemaphoreType.DMA((n,))
    out = pl.pallas_call(
        functools.partial(exchange_kernel, row_count, col_count, n_gz),
        out_shape=jax.ShapeDtypeStruct(shape, jnp.float32),
        in_specs=[vmem],
        out_specs=vmem,
        scratch_shapes=[
            pltpu.VMEM((n_gz - 1, n, part, width), jnp.float32),
            pltpu.VMEM((n, part, width), jnp.float32),
            pltpu.VMEM((n, part, width), jnp.float32),
            pair,
            pair,
            single,
            single,
            single,
            single,
            pair,
            pair,
        ],
        compiler_params=pltpu.CompilerParams(vmem_limit_bytes=VMEM_LIMIT, has_side_effects=True),
    )(term.reshape(shape))
    return out.reshape(total, width)


def on_device(blocks, coefficients, residuals):
    row_count = lax.axis_size("gx")
    col_count = lax.axis_size("gy")
    devices = row_count * col_count * lax.axis_size("gz")
    rows, slots, width = coefficients.shape
    scale = 1.0 / (rows * devices)
    nblock = G // width
    nsuper = nblock // 2
    used = panel_start(nblock, nblock) + nblock
    total = -(-used // (SUB * devices)) * SUB * devices
    vmem = pl.BlockSpec(memory_space=pltpu.VMEM)
    term = pl.pallas_call(
        functools.partial(gram_kernel, nblock, scale),
        out_shape=jax.ShapeDtypeStruct((total, width), jnp.float32),
        in_specs=[vmem] * 3,
        out_specs=vmem,
        scratch_shapes=[pltpu.VMEM((rows, G), jnp.bfloat16)],
        compiler_params=pltpu.CompilerParams(vmem_limit_bytes=VMEM_LIMIT),
    )(blocks, coefficients.transpose(1, 0, 2), residuals.reshape(1, rows))
    packed = exchange(term, row_count, col_count, lax.axis_size("gz"))
    place = jnp.stack([lax.axis_index("gx"), lax.axis_index("gy")]).astype(jnp.int32)
    per_row, per_col = nblock // row_count, nblock // col_count
    factor, answer = pl.pallas_call(
        functools.partial(factor_kernel, nblock),
        out_shape=(
            jax.ShapeDtypeStruct((per_row, width, per_col * width), jnp.float32),
            jax.ShapeDtypeStruct((nblock, width), jnp.float32),
        ),
        in_specs=[pl.BlockSpec(memory_space=pltpu.SMEM), pl.BlockSpec(memory_space=pl.ANY)],
        out_specs=(vmem, vmem),
        scratch_shapes=[
            pltpu.VMEM((nblock, G, width), jnp.float32),
            pltpu.VMEM((nsuper, SB, SB), jnp.float32),
            pltpu.VMEM((width, width), jnp.float32),
            pltpu.VMEM((width, width), jnp.float32),
            pltpu.VMEM((nsuper, SUB, SB), jnp.float32),
            pltpu.SemaphoreType.DMA((nblock + 1,)),
        ],
        compiler_params=pltpu.CompilerParams(vmem_limit_bytes=VMEM_LIMIT),
    )(place, packed)
    return (factor.reshape(1, per_row, width, 1, per_col, width), answer)


def solution(mesh):
    in_specs = (
        P(("gx", "gy", "gz"), None),
        P(("gx", "gy", "gz"), None, None),
        P(("gx", "gy", "gz")),
    )
    out_specs = (P("gx", None, None, "gy", None, None), P())
    return jax.shard_map(
        on_device, mesh=mesh, in_specs=in_specs, out_specs=out_specs, check_vma=False
    )
```
